32 devices in a mesh: dp: 4 (over y, x), tensor: 8 (over z, core).
Axes of the slice: x: 2, y: 2, z: 4, core: 2. Of those that a mesh axis runs over, the one named last changes fastest.
Arguments:
- noisy: bfloat16 [32, 256, 1152], P('dp', None, 'tensor'), may hold values from -6 to 6
- labels: int32 [32], P('dp'), may hold values from 0 to 999
- tsteps: int32 [32], P('dp'), may hold values from 0 to 999
- guide_index: int32 [32], P('dp'), may hold values from 0 to 31
- class_table: bfloat16 [1001, 1152], replicated, may hold values from -6 to 6
- time_table: bfloat16 [1000, 1152], replicated, may hold values from -6 to 6
- guide_table: bfloat16 [32, 1152], replicated, may hold values from -6 to 6
- guide_weights: float32 [32], replicated, may hold values from 0.5 to 4
- teacher_qkv: bfloat16 [1152, 3456], P(None, 'tensor'), may hold values from -0.1875 to 0.1875
- teacher_out: bfloat16 [1152, 1152], P('tensor'), may hold values from -0.1875 to 0.1875
- teacher_ada: bfloat16 [3, 1152, 1152], P(None, None, 'tensor'), may hold values from -0.1875 to 0.1875
- student_qkv: bfloat16 [1152, 3456], P(None, 'tensor'), may hold values from -0.1875 to 0.1875
- student_out: bfloat16 [1152, 1152], P('tensor'), may hold values from -0.1875 to 0.1875
- student_ada: bfloat16 [3, 1152, 1152], P(None, None, 'tensor'), may hold values from -0.1875 to 0.1875
Outputs:
- grad_qkv: float32 [1152, 3456], P('dp', 'tensor')
- grad_out: float32 [1152, 1152], P('tensor', 'dp')
- grad_ada: float32 [3, 1152, 1152], P(None, 'dp', 'tensor')
The draws below stay inside these ranges and needn't reach their ends.
All inputs are finite; a program needn't handle non-finite values.
Results may differ from the reference program's by a relative error of at most 0.034.
Values may be sent and summed in bfloat16 or wider, within the bound.
A program may use at most 128 MiB of HBM per device.

```python
import math
import jax
import jax.numpy as jnp
from jax import lax

D = 1152
HEADS = 16
HD = 72
CLASSES = 1000
L = 256
TSTEPS = 1000
GUIDES = 32
BATCH = 32
N_TENSOR = 8


def touch_ends(values, key, smallest, high):
    longest = values.shape.index(max(values.shape))
    spots = []
    for shift in (0, 1):
        where = [jax.random.randint(jax.random.fold_in(key, axis), (), 0, length) for axis, length in enumerate(values.shape)]
        where[longest] = (where[longest] + shift) % values.shape[longest]
        spots.append(tuple(where))
    return values.at[spots[0]].set(smallest).at[spots[1]].set(high)


def block_scale(stream_key, shape, pieces, low, largest):
    gain = 1.0
    for position, parts in pieces:
        steps = jax.random.uniform(jax.random.fold_in(jax.random.fold_in(stream_key, 6), position), (parts,), jnp.float32, low / len(pieces), largest / len(pieces))
        gain = gain * jnp.repeat(jnp.exp(steps), shape[position] // parts).reshape((-1,) + (1,) * (len(shape) - 1 - position))
    return gain


def normal_values(rng, dims, scale, limit, cuts=(), dtype=jnp.bfloat16):
    result = scale * jax.random.normal(rng, dims, jnp.float32)
    if cuts:
        result = result * block_scale(rng, dims, cuts, -0.22, 0.18)
    return jnp.clip(result, -limit, limit).astype(dtype)


def setup_inputs(seed: int = 0) -> dict:
    key_list = jax.random.split(jax.random.key(seed), 15)
    noisy = normal_values(key_list[0], (BATCH, L, D), 1.0, 6.0, ((0, 4), (2, 8)))
    labels = touch_ends(jax.random.randint(key_list[1], (BATCH,), 0, CLASSES), jax.random.fold_in(key_list[1], 1), 0, CLASSES - 1).astype(jnp.int32)
    tsteps = touch_ends(jax.random.randint(key_list[2], (BATCH,), 0, TSTEPS), jax.random.fold_in(key_list[2], 1), 0, TSTEPS - 1).astype(jnp.int32)
    guide_index = touch_ends(jax.random.randint(key_list[3], (BATCH,), 0, GUIDES), jax.random.fold_in(key_list[3], 1), 0, GUIDES - 1).astype(jnp.int32)
    class_table = normal_values(key_list[4], (CLASSES + 1, D), 1.0, 6.0)
    time_table = normal_values(key_list[5], (TSTEPS, D), 1.0, 6.0)
    guide_table = normal_values(key_list[6], (GUIDES, D), 1.0, 6.0)
    guide_weights = jnp.clip(jax.random.uniform(key_list[7], (GUIDES,), jnp.float32, 0.5, 4.0), 0.5, 4.0)
    teacher_qkv = normal_values(key_list[8], (D, 3 * D), D ** -0.5, 0.1875, ((1, 8),))
    teacher_out = normal_values(key_list[9], (D, D), D ** -0.5, 0.1875, ((0, 8),))
    teacher_ada = normal_values(key_list[10], (3, D, D), D ** -0.5, 0.1875, ((2, 8),))
    student_qkv = normal_values(key_list[11], (D, 3 * D), D ** -0.5, 0.1875, ((1, 8),))
    student_out = normal_values(key_list[12], (D, D), D ** -0.5, 0.1875, ((0, 8),))
    student_ada = normal_values(key_list[13], (3, D, D), D ** -0.5, 0.1875, ((2, 8),))
    return dict(noisy=noisy, labels=labels, tsteps=tsteps, guide_index=guide_index, class_table=class_table, time_table=time_table, guide_table=guide_table, guide_weights=guide_weights, teacher_qkv=teacher_qkv, teacher_out=teacher_out, teacher_ada=teacher_ada, student_qkv=student_qkv, student_out=student_out, student_ada=student_ada)


norm_eps = 1e-06

def round_trip(value):
    return lax.optimization_barrier(value.astype(jnp.bfloat16)).astype(jnp.float32)

def block_sum(left_rows, right_rows, block_count):
    inner_width = left_rows.shape[1] // block_count

    def add_block(block_idx, running):
        offset = (block_idx * inner_width).astype(jnp.int32)
        left_block = lax.dynamic_slice_in_dim(left_rows, offset, inner_width, 1)
        right_block = lax.dynamic_slice_in_dim(right_rows, offset, inner_width, 0)
        partial_value = jnp.dot(left_block, right_block, preferred_element_type=jnp.float32)
        return running + round_trip(partial_value)
    initial = jnp.zeros((left_rows.shape[0], right_rows.shape[1]), jnp.float32)
    return lax.fori_loop(0, block_count, add_block, initial)

def sample_probs(sample_qkv):
    queries = sample_qkv[:, :, 0].astype(jnp.float32)
    key_rows = sample_qkv[:, :, 1].astype(jnp.float32)
    scores = jnp.einsum('lhe,mhe->hlm', queries, key_rows) * (1.0 / math.sqrt(HD))
    exponent = jnp.exp(scores - lax.optimization_barrier(jnp.max(scores, axis=-1, keepdims=True)))
    return exponent / lax.optimization_barrier(jnp.sum(exponent, axis=-1, keepdims=True))

def attend_one(sample_qkv):
    attn_prob = sample_probs(sample_qkv)
    values = sample_qkv[:, :, 2].astype(jnp.float32)
    attn_mixed = jnp.einsum('hlm,mhe->lhe', round_trip(attn_prob), values)
    return attn_mixed.astype(jnp.bfloat16)

def attend_back(sample_pair):
    sample_qkv, grad_low = sample_pair
    attn_prob = sample_probs(sample_qkv)
    prob_low = round_trip(attn_prob)
    queries = sample_qkv[:, :, 0].astype(jnp.float32)
    key_rows = sample_qkv[:, :, 1].astype(jnp.float32)
    values = sample_qkv[:, :, 2].astype(jnp.float32)
    grad_mixed = grad_low.astype(jnp.float32)
    grad_probs = jnp.einsum('lhe,mhe->hlm', grad_mixed, values)
    row_delta = lax.optimization_barrier(jnp.sum(attn_prob * grad_probs, axis=-1, keepdims=True))
    grad_scores = round_trip(attn_prob * (grad_probs - row_delta) * (1.0 / math.sqrt(HD)))
    grad_query = jnp.einsum('hlm,mhe->lhe', grad_scores, key_rows)
    grad_keys = jnp.einsum('hlm,lhe->mhe', grad_scores, queries)
    grad_values = jnp.einsum('hlm,lhe->mhe', prob_low, grad_mixed)
    return jnp.stack([grad_query, grad_keys, grad_values], axis=2).astype(jnp.bfloat16)

def forward(normed, embed_act, qkv_weight, out_weight, ada_weight):
    batch_size = normed.shape[0]
    modulation = jnp.einsum('bd,kde->bke', embed_act.astype(jnp.float32), ada_weight.astype(jnp.float32))
    modulated = (normed.astype(jnp.float32) * (1.0 + modulation[:, 1][:, None]) + modulation[:, 0][:, None]).astype(jnp.bfloat16)
    qkv_sums = jnp.dot(modulated.reshape(-1, D), qkv_weight, preferred_element_type=jnp.float32)
    heads_qkv = qkv_sums.astype(jnp.bfloat16).reshape(batch_size, L, HEADS, 3, HD)
    attn_mixed = lax.map(attend_one, heads_qkv).reshape(-1, D)
    projected = block_sum(attn_mixed, out_weight, N_TENSOR).reshape(batch_size, L, D)
    branch = modulation[:, 2][:, None] * projected
    return (branch, modulated, heads_qkv, attn_mixed, projected, modulation)

def reference(noisy, labels, tsteps, guide_index, class_table, time_table, guide_table, guide_weights, teacher_qkv, teacher_out, teacher_ada, student_qkv, student_out, student_ada):
    batch_size = noisy.shape[0]
    signal = noisy.astype(jnp.float32)
    row_mean = lax.optimization_barrier(jnp.sum(signal, axis=2, keepdims=True)) / D
    row_var = lax.optimization_barrier(jnp.sum(signal * signal, axis=2, keepdims=True)) / D - row_mean * row_mean
    normed = ((signal - row_mean) * lax.rsqrt(row_var + norm_eps)).astype(jnp.bfloat16)
    time_embed = time_table[tsteps].astype(jnp.float32)
    cond_embed = class_table[labels].astype(jnp.float32) + time_embed
    null_embed = class_table[CLASSES].astype(jnp.float32)[None, :] + time_embed
    student_embed = cond_embed + guide_table[guide_index].astype(jnp.float32)
    cond_act = jax.nn.silu(cond_embed).astype(jnp.bfloat16)
    null_act = jax.nn.silu(null_embed).astype(jnp.bfloat16)
    student_act = jax.nn.silu(student_embed).astype(jnp.bfloat16)
    cond_result = forward(normed, cond_act, teacher_qkv, teacher_out, teacher_ada)
    null_result = forward(normed, null_act, teacher_qkv, teacher_out, teacher_ada)
    cond_update = round_trip(cond_result[0])
    null_update = round_trip(null_result[0])
    strength = guide_weights[guide_index][:, None, None]
    target = signal + ((1.0 + strength) * cond_update - strength * null_update)
    branch, modulated, heads_qkv, attn_mixed, projected, modulation = forward(normed, student_act, student_qkv, student_out, student_ada)
    cotangent = (signal + branch - target) * (1.0 / math.sqrt(batch_size * L))
    grad_gate = lax.optimization_barrier(jnp.sum(cotangent * projected, axis=1))
    grad_proj = (cotangent * modulation[:, 2][:, None]).astype(jnp.bfloat16).reshape(-1, D)
    grad_out = jnp.dot(attn_mixed.T, grad_proj, preferred_element_type=jnp.float32)
    grad_mixed = jnp.dot(grad_proj, student_out.T, preferred_element_type=jnp.float32)
    grad_low = grad_mixed.astype(jnp.bfloat16).reshape(batch_size, L, HEADS, HD)
    grad_qkv_act = lax.map(attend_back, (heads_qkv, grad_low)).reshape(-1, 3 * D)
    grad_qkv = jnp.dot(modulated.reshape(-1, D).T, grad_qkv_act, preferred_element_type=jnp.float32)
    grad_input = block_sum(grad_qkv_act, student_qkv.T, N_TENSOR).reshape(batch_size, L, D)
    grad_shift = lax.optimization_barrier(jnp.sum(grad_input, axis=1))
    grad_scale = lax.optimization_barrier(jnp.sum(grad_input * normed.astype(jnp.float32), axis=1))
    grad_modulation = jnp.stack([grad_shift, grad_scale, grad_gate], axis=1)
    grad_ada = jnp.einsum('bd,bke->kde', student_act.astype(jnp.float32), grad_modulation, precision=lax.Precision.HIGHEST)
    return (grad_qkv, grad_out, grad_ada)
```

```python
import math

import jax
import jax.numpy as jnp
from jax import lax
from jax.experimental import pallas as pl
from jax.experimental.pallas import tpu as pltpu
from jax.sharding import PartitionSpec as P

HD = 72


norm_eps = 1e-06


def lookup_rows(indices, table_rows):
    one_hot = (
        indices[:, None] == jnp.arange(table_rows.shape[0], dtype=jnp.int32)[None, :]
    ).astype(table_rows.dtype)
    return jnp.dot(one_hot, table_rows, preferred_element_type=jnp.float32)


def attend(qkv_sums, heads_here):
    batch_rows, seq_len = (qkv_sums.shape[0], qkv_sums.shape[1])
    heads_qkv = qkv_sums.astype(jnp.bfloat16).reshape(batch_rows, seq_len, heads_here, 3, HD)
    queries, key_rows, values = (
        heads_qkv[:, :, :, 0],
        heads_qkv[:, :, :, 1],
        heads_qkv[:, :, :, 2],
    )
    scores = jnp.einsum(
        "blhe,bmhe->bhlm", queries, key_rows, preferred_element_type=jnp.float32
    ) * (1.0 / math.sqrt(HD))
    exponent = jnp.exp(scores - jnp.max(scores, axis=-1, keepdims=True))
    attn_prob = exponent / jnp.sum(exponent, axis=-1, keepdims=True)
    prob_low = attn_prob.astype(jnp.bfloat16)
    attn_mixed = jnp.einsum("bhlm,bmhe->blhe", prob_low, values, preferred_element_type=jnp.float32)
    attn_mixed = attn_mixed.astype(jnp.bfloat16).reshape(batch_rows, seq_len, heads_here * HD)
    return (heads_qkv, attn_prob, prob_low, attn_mixed)


def attend_grad(heads_qkv, attn_prob, prob_low, grad_low):
    batch_rows, seq_len = (heads_qkv.shape[0], heads_qkv.shape[1])
    queries, key_rows, values = (
        heads_qkv[:, :, :, 0],
        heads_qkv[:, :, :, 1],
        heads_qkv[:, :, :, 2],
    )
    grad_probs = jnp.einsum("blhe,bmhe->bhlm", grad_low, values, preferred_element_type=jnp.float32)
    row_delta = jnp.sum(attn_prob * grad_probs, axis=-1, keepdims=True)
    grad_scores = (attn_prob * (grad_probs - row_delta) * (1.0 / math.sqrt(HD))).astype(
        jnp.bfloat16
    )
    grad_query = jnp.einsum(
        "bhlm,bmhe->blhe", grad_scores, key_rows, preferred_element_type=jnp.float32
    )
    grad_keys = jnp.einsum(
        "bhlm,blhe->bmhe", grad_scores, queries, preferred_element_type=jnp.float32
    )
    grad_values = jnp.einsum(
        "bhlm,blhe->bmhe", prob_low, grad_low, preferred_element_type=jnp.float32
    )
    grad_qkv_act = jnp.stack([grad_query, grad_keys, grad_values], axis=3).astype(jnp.bfloat16)
    return grad_qkv_act.reshape(batch_rows, seq_len, -1)


def modulate(normed, scale, shift):
    return (normed.astype(jnp.float32) * (1.0 + scale[:, None]) + shift[:, None]).astype(
        jnp.bfloat16
    )


def project_qkv(full_rows, qkv_weight):
    return jnp.einsum("bld,df->blf", full_rows, qkv_weight, preferred_element_type=jnp.float32)


def weight_grad_kernel(act_ref, grad_ref, scale_ref, shift_ref, weight_ref, sum_ref, mod_ref):
    @pl.when(pl.program_id(0) == 0)
    def _():
        sum_ref[...] = jnp.zeros_like(sum_ref)

    grads = grad_ref[0]
    over_tokens = lax.dot_general(
        grads,
        jnp.ones((grads.shape[0], 128), jnp.bfloat16),
        (((0,), (0,)), ((), ())),
        preferred_element_type=jnp.float32,
    )[:, :1]
    width = act_ref.shape[2]
    step = 384 if width % 384 == 0 else 128
    for start in range(0, width, step):
        cols = pl.ds(start, step)
        product = lax.dot_general(
            grads, act_ref[0, :, cols], (((0,), (0,)), ((), ())), preferred_element_type=jnp.float32
        )
        weight = weight_ref[:, cols].astype(jnp.float32)
        mod_ref[0, 0:1, cols] = jnp.sum(weight * over_tokens, axis=0, keepdims=True)
        mod_ref[0, 1:2, cols] = jnp.sum(weight * product, axis=0, keepdims=True)
        sum_ref[:, cols] += product * (1.0 + scale_ref[0, :, cols]) + over_tokens * shift_ref[
            0, :, cols
        ]


def weight_grad(normed, grad_qkv_act, scale, shift, weight_t):
    samples, seq_len, width = normed.shape
    columns = grad_qkv_act.shape[2]
    return pl.pallas_call(
        weight_grad_kernel,
        grid=(samples,),
        in_specs=[
            pl.BlockSpec((1, seq_len, width), lambda b: (b, 0, 0)),
            pl.BlockSpec((1, seq_len, columns), lambda b: (b, 0, 0)),
            pl.BlockSpec((1, 1, width), lambda b: (b, 0, 0)),
            pl.BlockSpec((1, 1, width), lambda b: (b, 0, 0)),
            pl.BlockSpec((columns, width), lambda b: (0, 0)),
        ],
        out_specs=[
            pl.BlockSpec((columns, width), lambda b: (0, 0)),
            pl.BlockSpec((1, 2, width), lambda b: (b, 0, 0)),
        ],
        out_shape=[
            jax.ShapeDtypeStruct((columns, width), jnp.float32),
            jax.ShapeDtypeStruct((samples, 2, width), jnp.float32),
        ],
        compiler_params=pltpu.CompilerParams(
            dimension_semantics=("arbitrary",), vmem_limit_bytes=32 * 1024 * 1024
        ),
        cost_estimate=pl.CostEstimate(
            flops=2 * samples * seq_len * width * columns,
            bytes_accessed=samples * seq_len * (width + columns) * 2 + width * columns * 6,
            transcendentals=0,
        ),
    )(normed, grad_qkv_act, scale[:, None], shift[:, None], weight_t)


def local(
    noisy,
    labels,
    tsteps,
    guide_index,
    class_table,
    time_table,
    guide_table,
    guide_weights,
    teacher_qkv,
    teacher_out,
    teacher_ada,
    student_qkv,
    student_out,
    student_ada,
):
    samples, seq_len, width_part = noisy.shape
    ways = lax.axis_size("tensor")
    groups = lax.axis_size("dp")
    me = lax.axis_index("tensor")
    model_width = width_part * ways
    batch_size = samples * groups
    wide_noisy = lax.all_gather(noisy, "tensor", axis=2, tiled=True)

    null_class = class_table.shape[0] - 1
    time_embed = lookup_rows(tsteps, time_table)
    cond_embed = lookup_rows(labels, class_table) + time_embed
    null_embed = class_table[null_class].astype(jnp.float32)[None, :] + time_embed
    guide_hot = guide_index[:, None] == jnp.arange(guide_table.shape[0], dtype=jnp.int32)[None, :]
    student_embed = cond_embed + jnp.dot(
        guide_hot.astype(jnp.bfloat16), guide_table, preferred_element_type=jnp.float32
    )
    strength = jnp.sum(jnp.where(guide_hot, guide_weights[None, :], 0.0), axis=1)
    cond_act = jax.nn.silu(cond_embed).astype(jnp.bfloat16)
    null_act = jax.nn.silu(null_embed).astype(jnp.bfloat16)
    student_act = jax.nn.silu(student_embed).astype(jnp.bfloat16)
    teacher_act = jnp.concatenate([cond_act, null_act], axis=0)
    mod_teacher = jnp.einsum(
        "bd,kde->kbe", teacher_act, teacher_ada, preferred_element_type=jnp.float32
    )
    mod_student = jnp.einsum(
        "bd,kde->kbe", student_act, student_ada, preferred_element_type=jnp.float32
    )
    mods = jnp.concatenate([mod_student, mod_teacher], axis=1).reshape(-1, width_part)
    wide_mods = gather_mods(mods).reshape(3, 3, samples, model_width)
    shift, scale, gate = wide_mods[0], wide_mods[1], wide_mods[2]

    teacher_out_full = lax.all_gather(teacher_out, "tensor", axis=0, tiled=True)
    student_out_full = lax.all_gather(student_out, "tensor", axis=0, tiled=True)

    signal = wide_noisy.astype(jnp.float32)
    row_mean = jnp.sum(signal, axis=2, keepdims=True) / model_width
    row_var = jnp.sum(signal * signal, axis=2, keepdims=True) / model_width - row_mean * row_mean
    normed = ((signal - row_mean) * lax.rsqrt(row_var + norm_eps)).astype(jnp.bfloat16)
    normed = lax.optimization_barrier(normed)

    heads_here = student_out.shape[0] // HD
    teacher_rows = jnp.concatenate(
        [modulate(normed, scale[1], shift[1]), modulate(normed, scale[2], shift[2])], axis=0
    )
    unused_qkv, unused_prob, unused_low, teacher_mixed = attend(
        project_qkv(teacher_rows, teacher_qkv), heads_here
    )
    student_rows = modulate(normed, scale[0], shift[0])
    heads_qkv, attn_prob, prob_low, student_mixed = attend(
        project_qkv(student_rows, student_qkv), heads_here
    )
    head_cols = heads_here * HD
    mixed = jnp.concatenate([student_mixed, teacher_mixed], axis=0).reshape(
        3, samples * seq_len, head_cols
    )
    mixed_rows = lax.all_to_all(mixed, "tensor", split_axis=1, concat_axis=2, tiled=True)

    row_count = samples * seq_len // ways
    run = min(row_count, seq_len)
    images = row_count // run
    first = me * row_count // seq_len
    own_gate = lax.dynamic_slice_in_dim(gate, first, images, axis=1)
    own_strength = lax.dynamic_slice_in_dim(strength, first, images, axis=0)[:, None]
    student_proj = jnp.dot(mixed_rows[0], student_out_full, preferred_element_type=jnp.float32)
    teacher_proj = jnp.einsum(
        "kre,ed->krd", mixed_rows[1:], teacher_out_full, preferred_element_type=jnp.float32
    ).reshape(2, images, run, model_width)
    student_proj = student_proj.reshape(images, run, model_width)
    scale_norm = 1.0 / math.sqrt(batch_size * seq_len)
    cotangent = scale_norm * (
        own_gate[0][:, None] * student_proj
        - ((1.0 + own_strength) * own_gate[1])[:, None] * teacher_proj[0]
        + (own_strength * own_gate[2])[:, None] * teacher_proj[1]
    )
    own_grad_gate = jnp.sum(cotangent * student_proj, axis=1)
    grad_proj = (
        (cotangent * own_gate[0][:, None]).astype(jnp.bfloat16).reshape(row_count, model_width)
    )
    grad_mixed_rows = lax.dot_general(
        grad_proj, student_out_full, (((1,), (1,)), ((), ())), preferred_element_type=jnp.float32
    ).astype(jnp.bfloat16)
    grad_low = lax.all_to_all(grad_mixed_rows, "tensor", split_axis=1, concat_axis=0, tiled=True)
    grad_low = grad_low.reshape(samples, seq_len, heads_here, HD)
    grad_out_part = lax.dot_general(
        mixed_rows[0], grad_proj, (((0,), (0,)), ((), ())), preferred_element_type=jnp.float32
    ).astype(jnp.bfloat16)
    grad_out = lax.psum_scatter(grad_out_part, "tensor", scatter_dimension=0, tiled=True)
    grad_out = lax.psum_scatter(grad_out, "dp", scatter_dimension=1, tiled=True).astype(jnp.float32)

    grad_qkv_act = attend_grad(heads_qkv, attn_prob, prob_low, grad_low)
    grad_qkv_t, grad_mod = weight_grad(normed, grad_qkv_act, scale[0], shift[0], student_qkv.T)
    grad_qkv = lax.psum_scatter(
        grad_qkv_t.T.astype(jnp.bfloat16), "dp", scatter_dimension=0, tiled=True
    ).astype(jnp.float32)

    grad_gate = lax.dynamic_update_slice_in_dim(
        jnp.zeros((samples, model_width), jnp.float32), own_grad_gate, first, axis=0
    )
    grad_mod = jnp.concatenate([grad_mod, grad_gate[:, None]], axis=1)
    act_all = lax.all_gather(student_act, "dp", axis=0, tiled=True)
    wide_grad = lax.psum_scatter(grad_mod, "tensor", scatter_dimension=2, tiled=True)
    wide_grad = lax.all_gather(wide_grad, "dp", axis=0, tiled=True)
    act_cols = model_width // groups
    own_act = lax.dynamic_slice_in_dim(act_all, lax.axis_index("dp") * act_cols, act_cols, axis=1)
    grad_ada = jnp.einsum(
        "bd,bke->kde",
        own_act.astype(jnp.float32),
        wide_grad,
        precision=lax.Precision.HIGHEST,
    )
    return (grad_qkv, grad_out, grad_ada)


def gather_mods(mods):
    gathered = lax.all_gather(mods, "tensor", axis=0)
    return gathered.transpose(1, 0, 2)


def solution(mesh):
    return jax.shard_map(
        local,
        mesh=mesh,
        in_specs=(
            P("dp", None, "tensor"),
            P("dp"),
            P("dp"),
            P("dp"),
            P(),
            P(),
            P(),
            P(),
            P(None, "tensor"),
            P("tensor", None),
            P(None, None, "tensor"),
            P(None, "tensor"),
            P("tensor", None),
            P(None, None, "tensor"),
        ),
        out_specs=(P("dp", "tensor"), P("tensor", "dp"), P(None, "dp", "tensor")),
        check_vma=False,
    )
```

```python
import functools
import math

import jax
import jax.numpy as jnp
from jax import lax
from jax.experimental import pallas as pl
from jax.experimental.pallas import tpu as pltpu
from jax.sharding import PartitionSpec as P

HD = 72


norm_eps = 1e-06


def lookup_rows(indices, table_rows):
    one_hot = (
        indices[:, None] == jnp.arange(table_rows.shape[0], dtype=jnp.int32)[None, :]
    ).astype(table_rows.dtype)
    return jnp.dot(one_hot, table_rows, preferred_element_type=jnp.float32)


def attend(qkv_sums, heads_here):
    batch_rows, seq_len = (qkv_sums.shape[0], qkv_sums.shape[1])
    heads_qkv = qkv_sums.astype(jnp.bfloat16).reshape(batch_rows, seq_len, heads_here, 3, HD)
    queries, key_rows, values = (
        heads_qkv[:, :, :, 0],
        heads_qkv[:, :, :, 1],
        heads_qkv[:, :, :, 2],
    )
    scores = jnp.einsum(
        "blhe,bmhe->bhlm", queries, key_rows, preferred_element_type=jnp.float32
    ) * (1.0 / math.sqrt(HD))
    exponent = jnp.exp(scores - jnp.max(scores, axis=-1, keepdims=True))
    attn_prob = exponent / jnp.sum(exponent, axis=-1, keepdims=True)
    prob_low = attn_prob.astype(jnp.bfloat16)
    attn_mixed = jnp.einsum("bhlm,bmhe->bhel", prob_low, values, preferred_element_type=jnp.float32)
    attn_mixed = attn_mixed.astype(jnp.bfloat16).reshape(batch_rows, heads_here * HD, seq_len)
    return (heads_qkv, attn_prob, prob_low, attn_mixed)


def attend_grad(heads_qkv, attn_prob, prob_low, grad_low):
    batch_rows, seq_len = (heads_qkv.shape[0], heads_qkv.shape[1])
    queries, key_rows, values = (
        heads_qkv[:, :, :, 0],
        heads_qkv[:, :, :, 1],
        heads_qkv[:, :, :, 2],
    )
    grad_probs = jnp.einsum("bhel,bmhe->bhlm", grad_low, values, preferred_element_type=jnp.float32)
    row_delta = jnp.sum(attn_prob * grad_probs, axis=-1, keepdims=True)
    grad_scores = (attn_prob * (grad_probs - row_delta) * (1.0 / math.sqrt(HD))).astype(
        jnp.bfloat16
    )
    grad_query = jnp.einsum(
        "bhlm,bmhe->blhe", grad_scores, key_rows, preferred_element_type=jnp.float32
    )
    grad_keys = jnp.einsum(
        "bhlm,blhe->bmhe", grad_scores, queries, preferred_element_type=jnp.float32
    )
    grad_values = jnp.einsum(
        "bhlm,bhel->bmhe", prob_low, grad_low, preferred_element_type=jnp.float32
    )
    grad_qkv_act = jnp.stack([grad_query, grad_keys, grad_values], axis=3).astype(jnp.bfloat16)
    return grad_qkv_act.reshape(batch_rows, seq_len, -1)


def exchange_kernel(axis, slots, count, *refs):
    sources, landings = refs[:count], refs[count : 2 * count]
    send_sem, recv_sem, own_sem = refs[2 * count :]
    ways = lax.axis_size(axis)
    me = lax.axis_index(axis)
    barrier = pltpu.get_barrier_semaphore()
    for hop in range(1, ways):
        peer = lax.rem(me + hop, ways)
        pl.semaphore_signal(
            barrier, inc=1, device_id={axis: peer}, device_id_type=pl.DeviceIdType.MESH
        )
    pl.semaphore_wait(barrier, ways - 1)
    copies = []
    for hop in range(1, ways):
        peer = lax.rem(me + hop, ways)
        for item in range(count):
            take, put = slots[item]
            copy = pltpu.make_async_remote_copy(
                src_ref=take(sources[item], peer),
                dst_ref=put(landings[item], me),
                send_sem=send_sem.at[item, hop - 1],
                recv_sem=recv_sem.at[item, hop - 1],
                device_id={axis: peer},
                device_id_type=pl.DeviceIdType.MESH,
            )
            copy.start()
            copies.append(copy)
    for item in range(count):
        take, put = slots[item]
        copy = pltpu.make_async_copy(
            take(sources[item], me), put(landings[item], me), own_sem.at[item]
        )
        copy.start()
        copies.append(copy)
    for copy in copies:
        copy.wait()


def exchange(axis, collective, arrays, shapes, slots):
    ways = lax.axis_size(axis)
    count = len(arrays)
    return pl.pallas_call(
        functools.partial(exchange_kernel, axis, slots, count),
        out_shape=[jax.ShapeDtypeStruct(s, a.dtype) for s, a in zip(shapes, arrays)],
        in_specs=[pl.BlockSpec(memory_space=pltpu.VMEM)] * count,
        out_specs=[pl.BlockSpec(memory_space=pltpu.VMEM)] * count,
        scratch_shapes=[
            pltpu.SemaphoreType.DMA((count, ways - 1)),
            pltpu.SemaphoreType.DMA((count, ways - 1)),
            pltpu.SemaphoreType.DMA((count,)),
        ],
        compiler_params=pltpu.CompilerParams(collective_id=collective, has_side_effects=True),
        cost_estimate=pl.CostEstimate(flops=0, bytes_accessed=40000000, transcendentals=0),
    )(*arrays)


def block_of(ref, index):
    return ref.at[index]


def whole_of(ref, index):
    return ref


def modulate(normed, scale, shift):
    return (normed.astype(jnp.float32) * (1.0 + scale[:, None]) + shift[:, None]).astype(
        jnp.bfloat16
    )


def project_qkv(full_rows, qkv_weight):
    return jnp.einsum("bld,df->blf", full_rows, qkv_weight, preferred_element_type=jnp.float32)


def weight_grad_kernel(act_ref, grad_ref, scale_ref, shift_ref, weight_ref, out_ref, mod_ref, sum_ref):
    @pl.when(pl.program_id(0) == 0)
    def _():
        sum_ref[...] = jnp.zeros_like(sum_ref)

    grads = grad_ref[0]
    over_tokens = lax.dot_general(
        grads,
        jnp.ones((grads.shape[0], 128), jnp.bfloat16),
        (((0,), (0,)), ((), ())),
        preferred_element_type=jnp.float32,
    )[:, :1]
    width = act_ref.shape[2]
    step = 384 if width % 384 == 0 else 128
    for start in range(0, width, step):
        cols = pl.ds(start, step)
        product = lax.dot_general(
            grads, act_ref[0, :, cols], (((0,), (0,)), ((), ())), preferred_element_type=jnp.float32
        )
        weight = weight_ref[:, cols].astype(jnp.float32)
        mod_ref[0, 0:1, cols] = jnp.sum(weight * over_tokens, axis=0, keepdims=True)
        mod_ref[0, 1:2, cols] = jnp.sum(weight * product, axis=0, keepdims=True)
        sum_ref[:, cols] += product * (1.0 + scale_ref[0, :, cols]) + over_tokens * shift_ref[
            0, :, cols
        ]

    @pl.when(pl.program_id(0) == pl.num_programs(0) - 1)
    def _():
        for start in range(0, width, step):
            cols = pl.ds(start, step)
            out_ref[cols, :] = sum_ref[:, cols].T.astype(out_ref.dtype)


def weight_grad(normed, grad_qkv_act, scale, shift, weight_t):
    samples, seq_len, width = normed.shape
    columns = grad_qkv_act.shape[2]
    return pl.pallas_call(
        weight_grad_kernel,
        grid=(samples,),
        in_specs=[
            pl.BlockSpec((1, seq_len, width), lambda b: (b, 0, 0)),
            pl.BlockSpec((1, seq_len, columns), lambda b: (b, 0, 0)),
            pl.BlockSpec((1, 1, width), lambda b: (b, 0, 0)),
            pl.BlockSpec((1, 1, width), lambda b: (b, 0, 0)),
            pl.BlockSpec((columns, width), lambda b: (0, 0)),
        ],
        out_specs=[
            pl.BlockSpec((width, columns), lambda b: (0, 0)),
            pl.BlockSpec((1, 2, width), lambda b: (b, 0, 0)),
        ],
        out_shape=[
            jax.ShapeDtypeStruct((width, columns), jnp.bfloat16),
            jax.ShapeDtypeStruct((samples, 2, width), jnp.float32),
        ],
        scratch_shapes=[pltpu.VMEM((columns, width), jnp.float32)],
        compiler_params=pltpu.CompilerParams(
            dimension_semantics=("arbitrary",), vmem_limit_bytes=32 * 1024 * 1024
        ),
        cost_estimate=pl.CostEstimate(
            flops=2 * samples * seq_len * width * columns,
            bytes_accessed=samples * seq_len * (width + columns) * 2 + width * columns * 6,
            transcendentals=0,
        ),
    )(normed, grad_qkv_act, scale[:, None], shift[:, None], weight_t)


def local(
    noisy,
    labels,
    tsteps,
    guide_index,
    class_table,
    time_table,
    guide_table,
    guide_weights,
    teacher_qkv,
    teacher_out,
    teacher_ada,
    student_qkv,
    student_out,
    student_ada,
):
    samples, seq_len, width_part = noisy.shape
    ways = lax.axis_size("tensor")
    groups = lax.axis_size("dp")
    me = lax.axis_index("tensor")
    model_width = width_part * ways
    batch_size = samples * groups
    wide_noisy = lax.all_gather(noisy, "tensor", axis=2, tiled=True)

    null_class = class_table.shape[0] - 1
    time_embed = lookup_rows(tsteps, time_table)
    cond_embed = lookup_rows(labels, class_table) + time_embed
    null_embed = class_table[null_class].astype(jnp.float32)[None, :] + time_embed
    guide_hot = guide_index[:, None] == jnp.arange(guide_table.shape[0], dtype=jnp.int32)[None, :]
    student_embed = cond_embed + jnp.dot(
        guide_hot.astype(jnp.bfloat16), guide_table, preferred_element_type=jnp.float32
    )
    strength = jnp.sum(jnp.where(guide_hot, guide_weights[None, :], 0.0), axis=1)
    cond_act = jax.nn.silu(cond_embed).astype(jnp.bfloat16)
    null_act = jax.nn.silu(null_embed).astype(jnp.bfloat16)
    student_act = jax.nn.silu(student_embed).astype(jnp.bfloat16)
    teacher_act = jnp.concatenate([cond_act, null_act], axis=0)
    mod_teacher = jnp.einsum(
        "bd,kde->kbe", teacher_act, teacher_ada, preferred_element_type=jnp.float32
    )
    mod_student = jnp.einsum(
        "bd,kde->kbe", student_act, student_ada, preferred_element_type=jnp.float32
    )
    mods = jnp.concatenate([mod_student, mod_teacher], axis=1).reshape(-1, width_part)
    wide_mods = gather_mods(mods).reshape(3, 3, samples, model_width)
    shift, scale, gate = wide_mods[0], wide_mods[1], wide_mods[2]

    teacher_out_full = lax.all_gather(teacher_out, "tensor", axis=0, tiled=True)
    student_out_full = lax.all_gather(student_out, "tensor", axis=0, tiled=True)

    signal = wide_noisy.astype(jnp.float32)
    row_mean = jnp.sum(signal, axis=2, keepdims=True) / model_width
    row_var = jnp.sum(signal * signal, axis=2, keepdims=True) / model_width - row_mean * row_mean
    normed = ((signal - row_mean) * lax.rsqrt(row_var + norm_eps)).astype(jnp.bfloat16)
    normed = lax.optimization_barrier(normed)

    heads_here = student_out.shape[0] // HD
    teacher_rows = jnp.concatenate(
        [modulate(normed, scale[1], shift[1]), modulate(normed, scale[2], shift[2])], axis=0
    )
    unused_qkv, unused_prob, unused_low, teacher_mixed = attend(
        project_qkv(teacher_rows, teacher_qkv), heads_here
    )
    student_rows = modulate(normed, scale[0], shift[0])
    heads_qkv, attn_prob, prob_low, student_mixed = attend(
        project_qkv(student_rows, student_qkv), heads_here
    )
    head_cols = heads_here * HD
    row_count = samples * seq_len // ways
    run = min(row_count, seq_len)
    images = row_count // run

    def rows_of(device):
        start = lax.rem(device * row_count, seq_len) if run < seq_len else 0
        if run < seq_len and run % 128 == 0:
            start = pl.multiple_of(start, 128)
        return pl.ds(device * row_count // seq_len, images), pl.ds(start, run)

    def take_tokens(ref, device):
        which, rows = rows_of(device)
        return ref.at[:, which, :, rows] if run < seq_len else ref.at[:, which]

    mixed = jnp.concatenate([student_mixed, teacher_mixed], axis=0).reshape(
        3, samples, head_cols, seq_len
    )
    (mixed_rows,) = exchange(
        "tensor",
        0,
        [mixed],
        [(ways, 3, images, head_cols, run)],
        [(take_tokens, block_of)],
    )
    first = me * row_count // seq_len
    own_gate = lax.dynamic_slice_in_dim(gate, first, images, axis=1)
    own_strength = lax.dynamic_slice_in_dim(strength, first, images, axis=0)[:, None]
    mixed_rows = mixed_rows.transpose(1, 2, 0, 3, 4).reshape(3, images, model_width, run)
    student_proj = jnp.einsum(
        "ier,ed->ird", mixed_rows[0], student_out_full, preferred_element_type=jnp.float32
    )
    teacher_proj = jnp.einsum(
        "kier,ed->kird", mixed_rows[1:], teacher_out_full, preferred_element_type=jnp.float32
    )
    scale_norm = 1.0 / math.sqrt(batch_size * seq_len)
    cotangent = scale_norm * (
        own_gate[0][:, None] * student_proj
        - ((1.0 + own_strength) * own_gate[1])[:, None] * teacher_proj[0]
        + (own_strength * own_gate[2])[:, None] * teacher_proj[1]
    )
    own_grad_gate = jnp.sum(cotangent * student_proj, axis=1)
    grad_proj = (cotangent * own_gate[0][:, None]).astype(jnp.bfloat16)
    grad_mixed_rows = (
        jnp.einsum("ed,ird->eir", student_out_full, grad_proj, preferred_element_type=jnp.float32)
        .astype(jnp.bfloat16)
        .reshape(ways, head_cols, images, run)
        .transpose(0, 2, 1, 3)
    )

    def put_heads(ref, device):
        which, rows = rows_of(device)
        return ref.at[which, :, rows] if run < seq_len else ref.at[which]

    (grad_low,) = exchange(
        "tensor",
        1,
        [grad_mixed_rows],
        [(samples, head_cols, seq_len)],
        [(block_of, put_heads)],
    )
    grad_low = grad_low.reshape(samples, heads_here, HD, seq_len)
    late_proj, grad_low = lax.optimization_barrier((grad_proj, grad_low))
    grad_out_part = jnp.einsum(
        "ier,ird->ed", mixed_rows[0], late_proj, preferred_element_type=jnp.float32
    ).astype(jnp.bfloat16)
    grad_out_rows = lax.psum_scatter(grad_out_part, "tensor", scatter_dimension=0, tiled=True)

    grad_qkv_act = attend_grad(heads_qkv, attn_prob, prob_low, grad_low)
    grad_qkv_part, grad_mod = weight_grad(
        normed, grad_qkv_act, scale[0], shift[0], student_qkv.T
    )
    grad_gate = lax.dynamic_update_slice_in_dim(
        jnp.zeros((samples, model_width), jnp.float32), own_grad_gate, first, axis=0
    )
    grad_mod = jnp.concatenate([grad_mod, grad_gate[:, None]], axis=1).reshape(
        samples * 3, ways, width_part
    )
    (mod_terms,) = exchange(
        "tensor",
        2,
        [grad_mod.transpose(1, 0, 2)],
        [(ways, samples * 3, width_part)],
        [(block_of, block_of)],
    )
    own_mod = jnp.sum(mod_terms, axis=0)
    depth = model_width // groups
    qkv_terms, out_terms, wide_grad, act_all = exchange(
        "dp",
        3,
        [
            grad_qkv_part.reshape(groups, depth, head_cols * 3),
            grad_out_rows.reshape(head_cols, groups, depth).transpose(1, 0, 2),
            own_mod,
            student_act,
        ],
        [
            (groups, depth, head_cols * 3),
            (groups, head_cols, depth),
            (groups, samples * 3, width_part),
            (groups, samples, model_width),
        ],
        [(block_of, block_of), (block_of, block_of), (whole_of, block_of), (whole_of, block_of)],
    )
    grad_qkv = jnp.sum(qkv_terms.astype(jnp.float32), axis=0)
    grad_out = jnp.sum(out_terms.astype(jnp.float32), axis=0)
    own_act = lax.dynamic_slice_in_dim(act_all, lax.axis_index("dp") * depth, depth, axis=2)
    grad_ada = jnp.einsum(
        "bd,bke->kde",
        own_act.reshape(batch_size, depth).astype(jnp.float32),
        wide_grad.reshape(batch_size, 3, width_part),
        precision=lax.Precision.HIGHEST,
    )
    return (grad_qkv, grad_out, grad_ada)


def gather_mods(mods):
    gathered = lax.all_gather(mods, "tensor", axis=0)
    return gathered.transpose(1, 0, 2)


def solution(mesh):
    return jax.shard_map(
        local,
        mesh=mesh,
        in_specs=(
            P("dp", None, "tensor"),
            P("dp"),
            P("dp"),
            P("dp"),
            P(),
            P(),
            P(),
            P(),
            P(None, "tensor"),
            P("tensor", None),
            P(None, None, "tensor"),
            P(None, "tensor"),
            P("tensor", None),
            P(None, None, "tensor"),
        ),
        out_specs=(P("dp", "tensor"), P("tensor", "dp"), P(None, "dp", "tensor")),
        check_vma=False,
    )
```
